32 devices in a mesh: hb: 4 (over y, core), row: 2 (over x), col: 4 (over z).
Axes of the slice: x: 2, y: 2, z: 4, core: 2. Of those that a mesh axis runs over, the one named last changes fastest.
Arguments:
- cell_state: float32 [256, 8, 256, 512], P('hb', None, 'row', 'col'), may hold values from -6 to 6
- normalizer: float32 [256, 8, 256], P('hb', None, 'row'), may hold values from 0.1 to 4
- stabilizer: float32 [256, 8, 16], P('hb', None, 'row'), may hold values from -5 to 120
- queries: float32 [256, 8, 256], P('hb', None, 'row'), may hold values from 0.0125 to 0.1125
- key_vectors: float32 [256, 8, 256], P('hb', None, 'row'), may hold values from -6 to 6
- token_value_vectors: float32 [256, 8, 512], P('hb', None, 'col'), may hold values from -6 to 6
- input_gate: float32 [256, 8], P('hb'), may hold values from -3 to 3
- forget_gate: float32 [256, 8], P('hb'), may hold values from -1 to 5
- output_gate_logits: float32 [256, 8, 512], P('hb', None, 'col'), may hold values from -6 to 6
- norm_gain: float32 [8, 512], P(None, 'col'), may hold values from 0.5 to 1.5
- out_weight: bfloat16 [8, 512, 4096], P('hb', 'col', 'row'), may hold values from -0.09375 to 0.09375
Outputs:
- layer_out: float32 [256, 4096], P('hb', 'row')
- readout: float32 [256, 8, 512], P('hb', None, 'col')
- refreshed_cell: float32 [256, 8, 256, 512], P('hb', None, 'row', 'col')
- new_normal: float32 [256, 8, 256], P('hb', None, 'row')
- new_stab: float32 [256, 8, 16], P('hb', None, 'row')
The draws below stay inside these ranges and needn't reach their ends.
All inputs are finite; a program needn't handle non-finite values.
Results may differ from the reference program's by a relative error of at most 0.0029.
Values may be sent and summed in bfloat16 or wider, within the bound.
A program may use at most 128 MiB of HBM per device.

```python
import math
import jax
import jax.numpy as jnp
from jax import lax

H = 8
DK = 256
DV = 512
D = 4096
RBLK = 16
NBLK = 16
BATCH = 256


def draw_stabilizer(key, part):
    offset_key, spread_key = jax.random.split(jax.random.fold_in(key, 7))
    offset = jax.random.uniform(offset_key, (BATCH, H, 1), jnp.float32, -1.0, 1.0)
    spread_factor = jax.random.uniform(spread_key, (BATCH, H, NBLK), jnp.float32, -1.5, 1.5)
    return offset + spread_factor


def level_of(rng, extent, shards, least, largest):
    factor_of, own = 1.0, jax.random.fold_in(rng, 6)
    for position, shards_of in shards:
        draws = jnp.exp(jax.random.uniform(jax.random.fold_in(own, position), (shards_of,), jnp.float32, least / len(shards), largest / len(shards)))
        factor_of = factor_of * jnp.repeat(draws, extent[position] // shards_of).reshape([-1 if axis == position else 1 for axis in range(len(extent))])
    return factor_of


def centred(rng, shape, scale, limit, cuts=(), kind=jnp.bfloat16):
    level = level_of(rng, shape, cuts, -0.22, 0.18) if cuts else 1.0
    array = jax.random.normal(rng, shape, jnp.float32) * scale * level
    return jnp.minimum(jnp.maximum(array, -limit), limit).astype(kind)


def setup_inputs(seed: int = 0) -> dict:
    streams_of = jax.random.split(jax.random.key(seed), 12)
    cell_state = centred(streams_of[0], (BATCH, H, DK, DV), 1.0, 6.0, ((0, 4), (2, 2), (3, 4)), jnp.float32)
    normalizer = jnp.clip(jnp.exp(math.log(4.0) - 3.6888794 * jax.random.uniform(streams_of[1], (BATCH, H, DK), jnp.float32) ** level_of(streams_of[1], (BATCH, H, DK), ((0, 4), (2, 2)), -0.2, 0.2)), 0.1, 4.0)
    stabilizer = draw_stabilizer(jax.random.fold_in(streams_of[11], 71), 0)
    queries = jnp.clip(0.0125 + 0.099999997 * jax.random.uniform(streams_of[3], (BATCH, H, DK), jnp.float32) ** level_of(streams_of[3], (BATCH, H, DK), ((0, 4), (2, 2)), -0.2, 0.2), 0.0125, 0.1125)
    key_vectors = centred(streams_of[4], (BATCH, H, DK), 1.0, 6.0, ((0, 4), (2, 2)), jnp.float32)
    token_value_vectors = centred(streams_of[5], (BATCH, H, DV), 1.0, 6.0, ((0, 4), (2, 4)), jnp.float32)
    input_gate = jnp.clip(jax.random.uniform(streams_of[6], (BATCH, H), jnp.float32, -3.0, 3.0) * level_of(streams_of[6], (BATCH, H), ((0, 4),), -0.4, 0.0), -3.0, 3.0)
    forget_gate = jnp.clip(-1.0 + 6.0 * jax.random.uniform(streams_of[7], (BATCH, H), jnp.float32) ** level_of(streams_of[7], (BATCH, H), ((0, 4),), -0.2, 0.2), -1.0, 5.0)
    output_gate_logits = centred(streams_of[8], (BATCH, H, DV), 1.0, 6.0, ((0, 4), (2, 4)), jnp.float32)
    norm_gain = jnp.clip(1.0 + 0.1 * jax.random.normal(streams_of[9], (H, DV), jnp.float32), 0.5, 1.5)
    out_weight = centred(streams_of[10], (H, DV, D), (H * DV) ** -0.5, 0.09375, ((0, 4), (1, 4), (2, 2)))
    return {"cell_state": cell_state, "normalizer": normalizer, "stabilizer": stabilizer, "queries": queries, "key_vectors": key_vectors, "token_value_vectors": token_value_vectors, "input_gate": input_gate, "forget_gate": forget_gate, "output_gate_logits": output_gate_logits, "norm_gain": norm_gain, "out_weight": out_weight}


def advance(cell, normal, stabs, query_row, token_key_row, value_row, in_gate, forget_pre):
    carried = jax.nn.log_sigmoid(forget_pre)[:, None] + stabs
    fresh = jnp.maximum(carried, in_gate[:, None])
    keep = jnp.repeat(jnp.exp(carried - fresh), RBLK, axis=1)
    admit = jnp.repeat(jnp.exp(in_gate[:, None] - fresh), RBLK, axis=1)
    scaled = token_key_row * DK ** (-0.5)
    refreshed_cell = keep[:, :, None] * cell + (admit * scaled)[:, :, None] * value_row[:, None, :]
    new_normal = keep * normal + admit * scaled
    top = lax.optimization_barrier(jnp.max(fresh, axis=1))
    weight_matrix = jnp.repeat(jnp.exp(fresh - top[:, None]), RBLK, axis=1) * query_row
    numerator = jnp.einsum('fdo,fd->fo', refreshed_cell, weight_matrix, precision=lax.Precision.HIGHEST)
    denom = lax.optimization_barrier(jnp.sum(new_normal * weight_matrix, axis=1))
    readout = numerator / jnp.maximum(jnp.abs(denom), jnp.exp(-top))[:, None]
    return (refreshed_cell, new_normal, fresh, readout)

def reference(cell_state, normalizer, stabilizer, queries, key_vectors, token_value_vectors, input_gate, forget_gate, output_gate_logits, norm_gain, out_weight):
    refreshed_cell, new_normal, new_stab, readout = lax.map(lambda packed: advance(*packed), (cell_state, normalizer, stabilizer, queries, key_vectors, token_value_vectors, input_gate, forget_gate))
    mean = lax.optimization_barrier(jnp.sum(readout, axis=2)) / DV
    var = lax.optimization_barrier(jnp.sum(readout * readout, axis=2)) / DV - mean * mean
    normed = (readout - mean[:, :, None]) * lax.rsqrt(var + 1e-06)[:, :, None]
    gated = (normed * norm_gain * jax.nn.sigmoid(output_gate_logits)).astype(jnp.bfloat16)
    layer_out = jnp.dot(gated.reshape(gated.shape[0], H * DV), out_weight.reshape(H * DV, D), preferred_element_type=jnp.float32)
    return (layer_out, readout, refreshed_cell, new_normal, new_stab)
```

```python
import functools

import jax
import jax.numpy as jnp
from jax import lax
from jax.experimental import pallas as pl
from jax.experimental.pallas import tpu as pltpu
from jax.sharding import PartitionSpec as P

DK = 256
DV = 512
RBLK = 16
PAIRS = 32
F32 = jnp.float32
BF16 = jnp.bfloat16


def combined_all(part, axis, combine):
    gathered = jax.tree.map(lambda a: lax.all_gather(a, axis), part)

    def take(source):
        return jax.tree.map(lambda a: lax.dynamic_index_in_dim(a, source, 0, False), gathered)

    return lax.fori_loop(
        1, lax.axis_size(axis), lambda source, state: combine(state, take(source)), take(0)
    )


def combine_pairs(left_pair, right_pair):
    joined = jnp.maximum(left_pair[0], right_pair[0])
    left_scale = jnp.exp(left_pair[0] - joined)
    right_scale = jnp.exp(right_pair[0] - joined)
    numerator = left_pair[1] * left_scale[:, :, None] + right_pair[1] * right_scale[:, :, None]
    denom = left_pair[2] * left_scale + right_pair[2] * right_scale
    return (joined, numerator, denom)


def cell_kernel(
    cell, norm, keep8, admit8, fresh8, queries, keys, values, new_cell, new_norm, numer, denom
):
    pairs, rows_k = norm.shape
    blocks = keep8.shape[1]
    lane = lax.broadcasted_iota(jnp.int32, (pairs, rows_k), 1) // RBLK

    def spread(small):
        wide = jnp.broadcast_to(small[:, 0:1], (pairs, rows_k))
        for block in range(1, blocks):
            wide = jnp.where(lane == block, small[:, block : block + 1], wide)
        return wide

    fresh = fresh8[...]
    top = jnp.max(fresh, axis=1, keepdims=True)
    keep = spread(keep8[...])
    write = spread(admit8[...]) * (keys[...] * DK ** (-0.5))
    weight = spread(jnp.exp(fresh - top)) * queries[...]
    normal = keep * norm[...] + write
    new_norm[...] = normal
    denom[...] = jnp.sum((normal * weight).T, axis=0, keepdims=True)[None]
    keep_t, write_t, weight_t = keep.T, write.T, weight.T
    for pair in range(pairs):
        column = slice(pair, pair + 1)
        fresh_cell = keep_t[:, column] * cell[pair] + write_t[:, column] * values[column, :]
        new_cell[pair] = fresh_cell
        numer[column, :] = jnp.sum(fresh_cell * weight_t[:, column], axis=0, keepdims=True)


def refresh(cell, norm, keep8, admit8, fresh8, queries, keys, values):
    count, pairs = cell.shape[0], PAIRS

    def rows_of(array):
        rest = array.shape[1:]
        return pl.BlockSpec((pairs,) + rest, lambda i, n=len(rest): (i,) + (0,) * n)

    args = (cell, norm, keep8, admit8, fresh8, queries, keys, values)
    return pl.pallas_call(
        cell_kernel,
        grid=(count // pairs,),
        in_specs=[rows_of(a) for a in args],
        out_specs=[
            rows_of(cell),
            rows_of(norm),
            rows_of(values),
            pl.BlockSpec((1, 1, pairs), lambda i: (i, 0, 0)),
        ],
        out_shape=[
            jax.ShapeDtypeStruct(cell.shape, F32),
            jax.ShapeDtypeStruct(norm.shape, F32),
            jax.ShapeDtypeStruct(values.shape, F32),
            jax.ShapeDtypeStruct((count // pairs, 1, pairs), F32),
        ],
        compiler_params=pltpu.CompilerParams(
            dimension_semantics=("arbitrary",), vmem_limit_bytes=24 << 20
        ),
        cost_estimate=pl.CostEstimate(
            flops=5 * cell.size, bytes_accessed=8 * cell.size, transcendentals=0
        ),
    )(*args)


def project_kernel(gated, *refs):
    n = lax.axis_size("col")
    hb = lax.axis_index("hb")
    col = lax.axis_index("col")
    weights, outs = refs[:-n], refs[-n:]
    depth, width = weights[0].shape
    chunk = width // n
    lhs = []
    for step in range(len(weights)):
        start = pl.multiple_of(lax.bitwise_xor(hb, jnp.int32(step)) * depth, depth)
        lhs.append(gated[:, pl.ds(start, depth)])
    for shift in range(n):
        start = pl.multiple_of(lax.rem(col + shift, n) * chunk, chunk)
        total = None
        for left, weight in zip(lhs, weights):
            term = jnp.dot(left, weight[:, pl.ds(start, chunk)], preferred_element_type=F32)
            total = term if total is None else total + term
        outs[shift][...] = total.astype(outs[shift].dtype)


def project(gated, weights):
    n = lax.axis_size("col")
    rows, width = gated.shape[0], weights[0].shape[1]
    vmem = pl.BlockSpec(memory_space=pltpu.VMEM)
    return pl.pallas_call(
        project_kernel,
        in_specs=[vmem] * (1 + len(weights)),
        out_specs=[vmem] * n,
        out_shape=[
            jax.ShapeDtypeStruct((rows, width // n), BF16 if shift else F32) for shift in range(n)
        ],
        compiler_params=pltpu.CompilerParams(vmem_limit_bytes=16 << 20),
        cost_estimate=pl.CostEstimate(
            flops=2 * gated.size * width, bytes_accessed=2 * gated.shape[1] * width, transcendentals=0
        ),
    )(gated, *weights)


def place_kernel(*refs):
    parts, out = refs[:-1], refs[-1]
    n = len(parts)
    col = lax.axis_index("col")
    chunk = parts[0].shape[1]
    for shift, part in enumerate(parts):
        start = pl.multiple_of(lax.rem(col + n - shift, n) * chunk, chunk)
        out[:, pl.ds(start, chunk)] = part[...].astype(F32)


def place(parts):
    rows, chunk = parts[0].shape
    vmem = pl.BlockSpec(memory_space=pltpu.VMEM)
    return pl.pallas_call(
        place_kernel,
        in_specs=[vmem] * len(parts),
        out_specs=vmem,
        out_shape=jax.ShapeDtypeStruct((rows, chunk * len(parts)), F32),
        compiler_params=pltpu.CompilerParams(vmem_limit_bytes=8 << 20),
    )(*parts)


def shifted(array, shift):
    n = lax.axis_size("col")
    return lax.ppermute(array, "col", [(i, (i + shift) % n) for i in range(n)])


def gathered_weights(weight):
    swap = lambda array, bit: lax.ppermute(array, "hb", [(i, i ^ bit) for i in range(4)])
    across = swap(weight, 2)
    return [weight, swap(weight, 1), across, swap(across, 1)]


def local(
    cell_state,
    normalizer,
    stabilizer,
    queries,
    key_vectors,
    token_value_vectors,
    input_gate,
    forget_gate,
    output_gate_logits,
    norm_gain,
    out_weight,
):
    seqs, heads, rows_k, cols_v = cell_state.shape
    count = seqs * heads
    flat = lambda a: a.reshape((count,) + a.shape[2:])
    carried = jax.nn.log_sigmoid(forget_gate)[:, :, None] + stabilizer
    fresh = jnp.maximum(carried, input_gate[:, :, None])
    keep8 = jnp.exp(carried - fresh)
    admit8 = jnp.exp(input_gate[:, :, None] - fresh)
    local_top = jnp.max(fresh, axis=2)
    own_kernel = rows_k % 128 == 0 and cols_v % 128 == 0 and count % PAIRS == 0 and heads % 8 == 0
    if own_kernel:
        new_cell, new_normal, numer, denom = refresh(
            flat(cell_state),
            flat(normalizer),
            flat(keep8),
            flat(admit8),
            flat(fresh),
            flat(queries),
            flat(key_vectors),
            flat(token_value_vectors),
        )
        refreshed_cell = new_cell.reshape(cell_state.shape)
        new_normal = new_normal.reshape(normalizer.shape)
        numerator = numer.reshape(seqs, heads, cols_v)
        denom = denom.reshape(seqs, heads)
    else:
        keep = jnp.repeat(keep8, RBLK, axis=2)
        write = jnp.repeat(admit8, RBLK, axis=2) * key_vectors * DK ** (-0.5)
        refreshed_cell = (
            keep[:, :, :, None] * cell_state
            + write[:, :, :, None] * token_value_vectors[:, :, None, :]
        )
        new_normal = keep * normalizer + write
        weight = jnp.repeat(jnp.exp(fresh - local_top[:, :, None]), RBLK, axis=2) * queries
        numerator = jnp.einsum(
            "bhkv,bhk->bhv", refreshed_cell, weight, precision=lax.Precision.HIGHEST
        )
        denom = jnp.sum(new_normal * weight, axis=2)
    if own_kernel and lax.axis_size("row") == 2:
        swap = [(0, 1), (1, 0)]
        small = jnp.stack([local_top, denom])
        other = lax.ppermute(numerator, "row", swap)
        other_small = lax.ppermute(small, "row", swap)
        first = lax.axis_index("row") == 0
        left = jnp.where(first, numerator, other)
        right = jnp.where(first, other, numerator)
        left_small = jnp.where(first, small, other_small)
        right_small = jnp.where(first, other_small, small)
        top, numerator, denom = combine_pairs(
            (left_small[0], left, left_small[1]), (right_small[0], right, right_small[1])
        )
    else:
        top, numerator, denom = combined_all(
            (local_top, numerator, denom), "row", combine_pairs
        )
    readout = numerator / jnp.maximum(jnp.abs(denom), jnp.exp(-top))[:, :, None]
    stats = jnp.stack([jnp.sum(readout, axis=2), jnp.sum(readout * readout, axis=2)])
    cols = lax.axis_size("col")
    arrived = [shifted(stats, shift) for shift in range(1, cols)]
    sums = functools.reduce(lambda a, b: a + b, arrived, stats)
    mean = sums[0] / DV
    var = sums[1] / DV - mean * mean
    normed = (readout - mean[:, :, None]) * lax.rsqrt(var + 1e-06)[:, :, None]
    gated = (normed * norm_gain * jax.nn.sigmoid(output_gate_logits)).astype(BF16)
    gated = gated.reshape(seqs, -1)
    out_cols = out_weight.shape[2]
    chunk = out_cols // cols
    if lax.axis_size("hb") == 4 and chunk % 128 == 0:
        outs = project(gated, gathered_weights(out_weight.reshape(-1, out_cols)))
        terms = [outs[0]] + [shifted(outs[shift], shift) for shift in range(1, cols)]
        mine = functools.reduce(lambda a, b: a + b, [t.astype(F32) for t in terms]).astype(BF16)
        layer_out = place([mine] + [shifted(mine, shift) for shift in range(1, cols)])
    else:
        partial_value = jnp.dot(
            gated,
            lax.all_gather(out_weight, "hb", axis=0, tiled=True).reshape(-1, out_cols),
            preferred_element_type=F32,
        )
        layer_out = lax.psum(partial_value, "col")
    return (layer_out, readout, refreshed_cell, new_normal, fresh)


def solution(mesh):
    placed = (
        P("hb", None, "row", "col"),
        P("hb", None, "row"),
        P("hb", None, "row"),
        P("hb", None, "row"),
        P("hb", None, "row"),
        P("hb", None, "col"),
        P("hb", None),
        P("hb", None),
        P("hb", None, "col"),
        P(None, "col"),
        P("hb", "col", "row"),
    )
    return jax.shard_map(
        local,
        mesh=mesh,
        in_specs=placed,
        out_specs=(
            P("hb", "row"),
            P("hb", None, "col"),
            P("hb", None, "row", "col"),
            P("hb", None, "row"),
            P("hb", None, "row"),
        ),
        check_vma=False,
    )
```
